32 devices in a mesh: grid: 16 (over z, x, core), band: 2 (over y).
Axes of the slice: x: 2, y: 2, z: 4, core: 2. Of those that a mesh axis runs over, the one named last changes fastest.
Arguments:
- left_bands: float32 [2, 8, 128, 128, 128], P(None, 'band', 'grid'), may hold values from -6 to 6
- right_bands: float32 [2, 4, 128, 128, 128], P(None, 'band', 'grid'), may hold values from -6 to 6
- sphere_index: int32 [16384], replicated, may hold values from 0 to 2097151, as said below
- right_order: int32 [4], replicated, may hold values from 0 to 3, each once
Outputs:
- pair_density: float32 [2, 8, 4, 16384], P(None, 'band', None, 'grid')
The draws below stay inside these ranges and needn't reach their ends.
Inputs may be any that keep to these rules, and one draw needn't show every extreme that they name: `sphere_index`: flat index (kz * 128 + ky) * 128 + kx; an index may repeat. In each aligned block of 1024 entries, at most 64 entries share one value of ky // 8, and some value is shared by exactly 64. `right_order`: each second band once.
All inputs are finite; a program needn't handle non-finite values.
Results may differ from the reference program's by a relative error of at most 0.00008.
Values sent between devices are 32-bit elements; how exact they have to be, the bound alone decides.
A program may use at most 256 MiB of HBM per device.

```python
import jax
import jax.numpy as jnp
from jax import lax

NG = 128
NX = 128
NGV = 16384
NL = 8
NR = 4
ZS = 8


def draw_sphere_index(key, part):
    devices = NG // ZS
    per_block = NGV // devices
    key_shift = jax.random.fold_in(key, 11)
    key_perm = jax.random.fold_in(key, 12)
    key_row = jax.random.fold_in(key, 13)
    key_plane = jax.random.fold_in(key, 14)
    key_column = jax.random.fold_in(key, 15)
    shifts = jax.random.randint(key_shift, (devices, 1), 0, devices)
    position = jnp.arange(per_block, dtype=jnp.int32)[None, :]
    source = (position + shifts) % devices
    block_keys = jax.random.split(key_perm, devices)
    orders = jax.vmap(lambda k: jax.random.permutation(k, per_block))(block_keys)
    source = jnp.take_along_axis(source, orders.astype(jnp.int32), axis=1).reshape(-1)
    wave_y = source * ZS + jax.random.randint(key_row, (NGV,), 0, ZS)
    wave_z = jax.random.randint(key_plane, (NGV,), 0, NG)
    wave_x = jax.random.randint(key_column, (NGV,), 0, NX)
    return ((wave_z * NG + wave_y) * NX + wave_x).astype(jnp.int32)


def levels(stream_key, shape, shards, low, top_value):
    def one(dim, parts):
        draws = jax.random.uniform(jax.random.fold_in(jax.random.fold_in(stream_key, 6), dim), (parts,), jnp.float32, low / len(shards), top_value / len(shards))
        return jnp.repeat(jnp.exp(draws), shape[dim] // parts).reshape((-1,) + (1,) * (len(shape) - dim - 1))

    factor_of = one(*shards[0])
    for cut in shards[1:]:
        factor_of = factor_of * one(*cut)
    return factor_of


def normal_values(stream_key, dims, scale, reach, cuts=(), kind=jnp.bfloat16):
    array = jax.random.normal(stream_key, dims, jnp.float32) * scale
    if len(cuts) > 0:
        array = levels(stream_key, dims, cuts, -0.22, 0.18) * array
    return jnp.clip(array, min=-reach, max=reach).astype(kind)


def setup_inputs(seed: int = 0) -> dict:
    key_list = jax.random.split(jax.random.key(seed), 5)
    return {
        "left_bands": normal_values(key_list[0], (2, NL, NG, NG, NX), 1.0, 6.0, ((1, 2), (2, 16)), jnp.float32),
        "right_bands": normal_values(key_list[1], (2, NR, NG, NG, NX), 1.0, 6.0, ((1, 2), (2, 16)), jnp.float32),
        "sphere_index": draw_sphere_index(jax.random.fold_in(key_list[4], 71), 0),
        "right_order": jax.random.permutation(key_list[3], NR).astype(jnp.int32),
    }


def reference(left_bands, right_bands, sphere_index, right_order):
    factor = 1.0 / (NG * NG * NX) ** 0.5

    def one_left(left_field):
        def one_right(column):
            right_field = lax.dynamic_index_in_dim(right_bands, column, 1, keepdims=False)
            real_part = left_field[0] * right_field[0] + left_field[1] * right_field[1]
            imag_part = left_field[0] * right_field[1] - left_field[1] * right_field[0]
            spectrum = jnp.fft.fftn(real_part + 1j * imag_part)
            picked = spectrum.reshape(-1)[sphere_index]
            return jnp.stack([jnp.real(picked), jnp.imag(picked)]).astype(jnp.float32) * factor

        return lax.map(one_right, right_order)

    result = lax.map(one_left, jnp.moveaxis(left_bands, 1, 0))
    return jnp.transpose(result, (2, 0, 1, 3))
```

```python
import math

import jax
import jax.numpy as jnp
import numpy as np
from jax import lax
from jax.experimental import pallas as pl
from jax.experimental.pallas import tpu as pltpu
from jax.sharding import PartitionSpec as P

HIGH = lax.Precision.HIGH
HIGHEST = lax.Precision.HIGHEST
F32 = jnp.float32
BF16 = jnp.bfloat16


def swapped(block, axis):
    count = lax.axis_size(axis)
    return lax.ppermute(block, axis, [(k, k ^ 1) for k in range(count)])


def dft_tables(length):
    counter = jnp.arange(length, dtype=jnp.int32)
    angles = (counter[:, None] * counter[None, :] % length).astype(F32) * (2.0 * math.pi / length)
    return (jnp.cos(angles), jnp.sin(angles))


def complex_matrix(length):
    cosine, sine = dft_tables(length)
    return jnp.concatenate(
        [jnp.concatenate([cosine, -sine], 1), jnp.concatenate([sine, cosine], 1)], 0
    ).reshape(2, length, 2, length)


def split(value):
    high = lax.reduce_precision(value, 8, 7)
    return high.astype(BF16), (value - high).astype(BF16)


def plan(sphere_index, grid, nx, n_dev):
    rows = grid // n_dev
    per = sphere_index.shape[0] // n_dev
    slots = max(1, per // n_dev)
    wave_z = sphere_index // (grid * nx)
    wave_y = sphere_index // nx % grid
    wave_x = sphere_index % nx
    source = (wave_y // rows).reshape(n_dev, per)
    onehot = (source[:, :, None] == jnp.arange(n_dev, dtype=jnp.int32)).astype(BF16)
    before = jnp.tril(jnp.ones((per, per), BF16), -1)
    counts = jnp.einsum("ij,bjs->bis", before, onehot, preferred_element_type=F32)
    rank = jnp.sum(counts * onehot, axis=2).astype(jnp.int32)
    slot = source * slots + rank
    column = (wave_y % rows) * nx + wave_x
    packed = (wave_z * (rows * nx) + column).reshape(n_dev, per)
    target = jnp.arange(n_dev * slots, dtype=jnp.int32)
    chosen = jnp.sum(
        jnp.where(slot[:, :, None] == target[None, None, :], packed[:, :, None] + 1, 0), axis=1
    ) - 1
    bits = n_dev.bit_length() - 1
    if n_dev == 1 << bits:
        chosen = chosen.reshape((2,) * bits + (n_dev * slots,))
        chosen = chosen.transpose(tuple(range(bits))[::-1] + (bits,))
    chosen = chosen.reshape(n_dev, n_dev, slots).transpose(1, 0, 2).reshape(n_dev, n_dev * slots)
    return chosen, slot


def select_body(field_ref, col_ref, cos_ref, sin_ref, out_ref, parts_ref):
    count, rows, nx = field_ref.shape
    planes = cos_ref.shape[1]
    points = col_ref.shape[2]
    flat = field_ref.reshape(count * rows, nx)
    for row in range(rows):
        value = flat[pl.ds(row, count, stride=rows), :]
        high = value.astype(BF16)
        low = (value - high.astype(F32)).astype(BF16)
        parts_ref[0:count, row * nx : (row + 1) * nx] = high
        parts_ref[count : 2 * count, row * nx : (row + 1) * nx] = low
    tile = min(points, 256)

    def step(index, carry):
        span = pl.ds(pl.multiple_of(index * tile, tile), tile)
        col = col_ref[0, :, span]
        place = lax.broadcasted_iota(jnp.int32, (rows * nx, tile), 0)
        hot = jnp.where(place == col, 1.0, 0.0).astype(BF16)
        both = jnp.dot(parts_ref[...], hot, preferred_element_type=F32)
        got = (both[:count] + both[count:]).reshape(2, count // (2 * planes), planes, tile)
        cosine, sine = cos_ref[0, :, span][None], sin_ref[0, :, span][None]
        real = jnp.sum(got[0] * cosine + got[1] * sine, axis=1)
        imag = jnp.sum(got[1] * cosine - got[0] * sine, axis=1)
        out_ref[0, :, span] = jnp.concatenate([real, imag], axis=0)
        return carry

    lax.fori_loop(0, points // tile, step, 0)


def select_sum(field, col, cos_z, sin_z):
    two, pairs, planes, ng, nx = field.shape
    groups, points = col.shape
    rows = ng // groups
    if rows % 8 == 0 and planes % 8 == 0 and nx % 128 == 0 and points % 256 == 0:
        count = two * pairs * planes
        flops = 4 * count * rows * nx * points * groups
        return pl.pallas_call(
            select_body,
            grid=(groups,),
            in_specs=[
                pl.BlockSpec((count, rows, nx), lambda g: (0, g, 0)),
                pl.BlockSpec((1, 1, points), lambda g: (g, 0, 0)),
                pl.BlockSpec((1, planes, points), lambda g: (g, 0, 0)),
                pl.BlockSpec((1, planes, points), lambda g: (g, 0, 0)),
            ],
            out_specs=pl.BlockSpec((1, 2 * pairs, points), lambda g: (g, 0, 0)),
            out_shape=jax.ShapeDtypeStruct((groups, 2 * pairs, points), F32),
            scratch_shapes=[pltpu.VMEM((2 * count, rows * nx), BF16)],
            cost_estimate=pl.CostEstimate(
                flops=flops, bytes_accessed=4 * count * ng * nx, transcendentals=0
            ),
        )(field.reshape(count, ng, nx), col[:, None, :], cos_z, sin_z)
    high, low = split(field.reshape(2, pairs, planes, groups, rows * nx))
    place = jnp.arange(rows * nx, dtype=jnp.int32)[None, :, None]
    hot = (place == col[:, None, :]).astype(BF16)
    form = "dpzsc,scq->sdpzq"
    got = jnp.einsum(form, high, hot, preferred_element_type=F32) + jnp.einsum(
        form, low, hot, preferred_element_type=F32
    )
    c, s = cos_z[:, None], sin_z[:, None]
    real = jnp.sum(got[:, 0] * c + got[:, 1] * s, axis=2)
    imag = jnp.sum(got[:, 1] * c - got[:, 0] * s, axis=2)
    return jnp.concatenate([real, imag], axis=1)


def halved(part, me, n_dev, bit):
    half = part.shape[2] // 2
    lower, upper = part[:, :, :half], part[:, :, half:]
    mine = me // (1 << bit) % 2 == 1
    route = [(k, k ^ (1 << bit)) for k in range(n_dev)]
    arrived = lax.ppermute(jnp.where(mine, lower, upper), "grid", route)
    return jnp.where(mine, upper, lower) + arrived


def summed_over_grid(part, me, n_dev, done):
    bits = n_dev.bit_length() - 1
    if n_dev == 1 << bits:
        for bit in range(done, bits):
            part = halved(part, me, n_dev, bit)
        return part
    groups, values, points = part.shape
    part = part.reshape(groups, values, n_dev, points // n_dev).transpose(2, 0, 1, 3)
    return lax.psum_scatter(part, "grid", scatter_dimension=0, tiled=False)


LANES = 128
SUBLANES = 8
MESH = pl.DeviceIdType.MESH


def constant_matrix(length):
    counter = np.arange(length)
    angles = (counter[:, None] * counter[None, :] % length) * (2.0 * math.pi / length)
    cosine, sine = np.cos(angles), np.sin(angles)
    return np.concatenate(
        [np.concatenate([cosine, -sine], 1), np.concatenate([sine, cosine], 1)], 0
    ).astype(np.float32)


def constant_split(value):
    high = value.astype(BF16)
    return high, (value - high.astype(np.float32)).astype(BF16)


def dot(a, b):
    return jnp.dot(a, b, preferred_element_type=F32)


def parts(value):
    high = value.astype(BF16)
    return high, (value - high.astype(F32)).astype(BF16)


def lane_gather(value, index):
    return jnp.take_along_axis(value, index, axis=1, mode="promise_in_bounds")


def fused_body(
    n_dev,
    left_hbm, right_hbm, index_ref, pos_ref, upper_ref, table_ref, wyh, wyl, wxh, wxl,
    out_ref,
    left, right, field, acc, came, came2, final, plan_kx, plan_ky, cos_z, sin_z, own_slot,
    sem_in, sem_xs, sem_xr, sem_1s, sem_1r, sem_2s, sem_2r, sem_3s, sem_3r,
):
    nl, planes, ng, nx = left.shape[1:]
    own = right_hbm.shape[1]
    nr = right.shape[1]
    rows = ng // n_dev
    chips = n_dev // 2
    pitch = field.shape[2] // (2 * nl)
    slots = LANES // 2
    blocks = index_ref.shape[0] // n_dev
    spans = sem_xs.shape[0] // own
    step = planes // spans
    me = lax.axis_index("grid")
    band = lax.axis_index("band")
    core, chip = lax.rem(me, 2), me // 2
    partner = me + 1 - 2 * core

    def at(grid):
        return {"grid": grid, "band": band}

    barrier = pltpu.get_barrier_semaphore()
    pl.semaphore_signal(
        barrier, inc=1, device_id={"grid": me, "band": 1 - band}, device_id_type=MESH
    )
    pl.semaphore_signal(barrier, inc=1, device_id=at(partner), device_id_type=MESH)
    for o in range(1, chips):
        other = lax.rem(chip + o, chips) * 2 + core
        pl.semaphore_signal(barrier, inc=1, device_id=at(other), device_id_type=MESH)
    load_right = pltpu.make_async_copy(right_hbm, right.at[:, 0:own], sem_in.at[0])
    load_left = pltpu.make_async_copy(left_hbm, left, sem_in.at[1])
    load_right.start()
    load_left.start()
    pl.semaphore_wait(barrier, chips + 1)

    def remote(src, dst, send, recv, where):
        return pltpu.make_async_remote_copy(
            src_ref=src, dst_ref=dst, send_sem=send, recv_sem=recv,
            device_id=where, device_id_type=MESH,
        )

    def swap(m, span):
        part = pl.ds(span * step, step)
        k = m * spans + span
        return remote(
            right_hbm.at[:, m, part], right.at[:, own + m, part],
            sem_xs.at[k], sem_xr.at[k], {"grid": me, "band": 1 - band},
        )

    for m in range(own):
        for span in range(spans):
            swap(m, span).start()

    bit_x, bit_y = nx.bit_length() - 1, ng.bit_length() - 1
    bit_r = rows.bit_length() - 1
    iota_s = lax.broadcasted_iota(jnp.int32, (n_dev, LANES), 0)
    iota_r = lax.broadcasted_iota(jnp.int32, (slots, LANES), 0)
    iota_p = lax.broadcasted_iota(jnp.int32, (planes, LANES), 0)

    def plan_block(t):
        value = index_ref[pl.ds(pl.multiple_of(t * blocks, blocks), blocks), :]
        source = (value >> (bit_x + bit_r)) & (n_dev - 1)
        ky = (value >> bit_x) & (rows - 1)
        kx = value & (nx - 1)
        kz = value >> (bit_x + bit_y)
        masks = [
            jnp.broadcast_to(source[c : c + 1], (n_dev, LANES)) == iota_s for c in range(blocks)
        ]
        hot = jnp.concatenate([jnp.where(k, 1.0, 0.0) for k in masks], 0).astype(BF16)
        prefix = dot(hot, upper_ref[...])
        carry = jnp.zeros((n_dev, LANES), F32)
        left_side, right_side, ranks = [], [], []
        for c in range(blocks):
            mine = prefix[c * n_dev : (c + 1) * n_dev]
            count = mine[:, :LANES] + carry
            carry = carry + mine[:, LANES:]
            rank = jnp.sum(jnp.where(masks[c], count, 0.0), axis=0, keepdims=True)
            rank = rank.astype(jnp.int32)
            ranks.append(rank)
            wide = [
                jnp.where(
                    masks[c],
                    jnp.broadcast_to(v[c : c + 1].astype(F32), (n_dev, LANES)), 0.0
                )
                for v in (kz, ky, kx)
            ]
            left_side.append(jnp.concatenate(wide, 0))
            right_side.append(
                jnp.where(jnp.broadcast_to(rank, (slots, LANES)) == iota_r, 1.0, 0.0)
            )
        own_slot[t, 0] = source
        own_slot[t, 1] = jnp.concatenate(ranks, 0)
        a = jnp.concatenate(left_side, 1).astype(BF16)
        b = jnp.concatenate(right_side, 1).astype(BF16)
        return lax.dot_general(a, b, (((1,), (1,)), ((), ())), preferred_element_type=F32)

    def plan_chip(ch, carry):
        both = jnp.concatenate([plan_block(2 * ch), plan_block(2 * ch + 1)], 1)
        both = both.astype(jnp.int32)
        kz = both[0:n_dev]
        plan_ky[ch] = both[n_dev : 2 * n_dev]
        plan_kx[ch] = both[2 * n_dev : 3 * n_dev]
        for g in range(n_dev):
            turn = jnp.broadcast_to(kz[g : g + 1], (planes, LANES)) * (me * planes + iota_p)
            turn = turn & (ng - 1)
            cos_z[ch, g] = lane_gather(table_ref[0], turn)
            sin_z[ch, g] = lane_gather(table_ref[1], turn)
        return carry

    lax.fori_loop(0, chips, plan_chip, 0)

    def transform(m, z, q, buf):
        r0, r1 = right[0, m, z], right[1, m, z]
        real, imag = [], []
        for e in range(2):
            l0, l1 = left[0, 2 * q + e, z], left[1, 2 * q + e, z]
            real.append(l0 * r0 + l1 * r1)
            imag.append(l0 * r1 - l1 * r0)
        pair = jnp.concatenate([jnp.concatenate(real, 1), jnp.concatenate(imag, 1)], 0)
        high, low = parts(pair)
        y = dot(wyh[...], high) + dot(wyl[...], high) + dot(wyh[...], low)
        lines = jnp.concatenate(
            [
                jnp.concatenate([y[:ng, e * nx : (e + 1) * nx], y[ng:, e * nx : (e + 1) * nx]], 1)
                for e in range(2)
            ],
            0,
        )
        high, low = parts(lines)
        x = dot(high, wxh[...]) + dot(low, wxh[...]) + dot(high, wxl[...])
        for d in range(2):
            for e in range(2):
                start = pl.multiple_of((d * nl + 2 * q + e) * pitch, SUBLANES)
                field[buf, z, pl.ds(start, ng), :] = x[
                    e * ng : (e + 1) * ng, d * nx : (d + 1) * nx
                ]

    sign = jnp.where(lax.broadcasted_iota(jnp.int32, (2 * nl, LANES), 0) < nl, 1.0, -1.0)

    def choose(items, bits):
        for bit in bits:
            items = [jnp.where(bit, items[2 * k + 1], items[2 * k]) for k in range(len(items) // 2)]
        return items[0]

    def bits_of(value, count, shape):
        value = jnp.broadcast_to(value, shape)
        return [((value >> i) & 1) == 1 for i in range(count)]

    def gather_group(m, g, buf, zs, add):
        half, inner = g // (n_dev // 2), lax.rem(g, n_dev // 2)
        shape = (2 * nl, LANES)
        for ch in range(chips):
            index = jnp.broadcast_to(plan_kx[ch, pl.ds(g, 1), :], shape)
            bits = bits_of(plan_ky[ch, pl.ds(g, 1), :], bit_r, shape)
            even = odd = None
            for z in zs:
                got = choose(
                    [
                        lane_gather(
                            field[buf, z, pl.ds(g * rows + k, 2 * nl, stride=pitch), :], index
                        )
                        for k in range(rows)
                    ],
                    bits,
                )
                c = jnp.broadcast_to(cos_z[ch, g, pl.ds(z, 1), :], shape)
                s = jnp.broadcast_to(sin_z[ch, g, pl.ds(z, 1), :], shape)
                even = got * c if even is None else even + got * c
                odd = got * s if odd is None else odd + got * s
            total = even + sign * pltpu.roll(odd, nl, 0)
            if add:
                total = total + acc[m, half, ch, inner]
            acc[m, half, ch, inner] = total

    def send1(m):
        return remote(
            acc.at[m, 1 - core], came.at[m], sem_1s.at[m], sem_1r.at[m], at(partner)
        )

    def send2(m, o):
        other = lax.rem(chip + o, chips)
        return remote(
            acc.at[m, core, other], came2.at[m, o - 1],
            sem_2s.at[m, o - 1], sem_2r.at[m, o - 1], at(other * 2 + core),
        )

    def send3(m):
        return remote(
            final.at[m, core], final.at[m, core], sem_3s.at[m], sem_3r.at[m], at(partner)
        )

    def stage2(m):
        send1(m).wait_recv()

        def add(ch, carry):
            acc[m, core, ch] = acc[m, core, ch] + came[m, ch]
            return carry

        lax.fori_loop(0, chips, add, 0)
        for o in range(1, chips):
            send2(m, o).start()

    def stage3(m):
        for o in range(1, chips):
            send2(m, o).wait_recv()
        total = acc[m, core, chip]
        for o in range(1, chips):
            total = total + came2[m, o - 1]
        final[m, core] = total
        send3(m).start()

    load_right.wait()
    load_left.wait()
    half = nl // 2

    def first(z, carry):
        for q in range(half):
            transform(0, z, q, 0)
        return carry

    lax.fori_loop(0, planes, first, 0)

    def both(m, buf):
        def run(g, carry):
            gather_group(m, g, buf, range(planes), False)
            transform(m + 1, g // half, lax.rem(g, half), 1 - buf)
            return carry

        lax.fori_loop(0, n_dev, run, 0)

    def only(m, buf):
        def run(g, carry):
            gather_group(m, g, buf, range(planes), False)
            return carry

        lax.fori_loop(0, n_dev, run, 0)

    both(0, 0)
    send1(0).start()
    for span in range(spans):
        swap(0, span).wait_recv()
    both(1, 1)
    send1(1).start()
    stage2(0)
    only(2, 0)
    send1(2).start()
    stage2(1)
    stage3(0)

    def clear(i, carry):
        acc[3, i // chips, lax.rem(i, chips)] = jnp.zeros(acc.shape[3:], F32)
        return carry

    lax.fori_loop(0, 2 * chips, clear, 0)

    def tail(span, carry):
        swap(1, span).wait_recv()

        def work(k, carry):
            for q in range(half):
                transform(3, span * step + k, q, 1)
            return carry

        lax.fori_loop(0, step, work, 0)

        def run(k, carry):
            for e in range(4):
                gather_group(
                    3, k * 4 + e, 1, [span * step + z for z in range(step)], True
                )
            return carry

        lax.fori_loop(0, n_dev // 4, run, 0)
        return carry

    lax.fori_loop(0, spans, tail, 0)
    send1(3).start()
    stage2(2)
    stage3(1)
    stage2(3)
    stage3(2)
    stage3(3)
    for m in range(nr):
        send3(m).wait_recv()

    source, rank = own_slot[me, 0], own_slot[me, 1]
    shape = (2 * nl, LANES)
    for c in range(blocks):
        index = jnp.broadcast_to(rank[c : c + 1] + core * slots, shape)
        bits = bits_of(source[c : c + 1], n_dev.bit_length() - 1, shape)
        got = [
            choose(
                [
                    lane_gather(final[m, g // chips, g % chips], index)
                    for g in range(n_dev)
                ],
                bits,
            )
            for m in range(nr)
        ]
        for j in range(nr):
            pos = jnp.broadcast_to(pos_ref[j : j + 1, :], shape)
            value = got[0]
            for m in range(1, nr):
                value = jnp.where(pos == m, got[m], value)
            out_ref[j, :, c * LANES : (c + 1) * LANES] = value

    for m in range(own):
        for span in range(spans):
            swap(m, span).wait_send()
    for m in range(nr):
        send1(m).wait_send()
        for o in range(1, chips):
            send2(m, o).wait_send()
        send3(m).wait_send()


def fused_fits(left_bands, right_bands, sphere_index, n_dev):
    two, nl, zs, ng, nx = left_bands.shape
    per = sphere_index.shape[0] // n_dev
    return (
        ng == nx == LANES
        and zs * n_dev == ng
        and zs == SUBLANES
        and 2 * nl == SUBLANES
        and right_bands.shape[1] == 2
        and lax.axis_size("band") == 2
        and per == SUBLANES * LANES
        and 2 * (per // n_dev) == LANES
        and n_dev == 2 * SUBLANES
    )


def fused(left_bands, right_bands, sphere_index, right_order):
    n_dev = lax.axis_size("grid")
    two, nl, zs, ng, nx = left_bands.shape
    own = right_bands.shape[1]
    nr = right_order.shape[0]
    chips = n_dev // 2
    per = sphere_index.shape[0] // n_dev
    spans = 4
    pitch = ng + SUBLANES
    scale = 1.0 / (ng * ng * nx) ** 0.5
    position = (right_order - lax.axis_index("band") * own) % nr
    position = jnp.broadcast_to(position.astype(jnp.int32)[:, None], (nr, LANES))
    upper = np.concatenate([np.triu(np.ones((LANES, LANES)), 1), np.ones((LANES, LANES))], 1)
    angle = np.arange(ng) * (2.0 * math.pi / ng)
    table = np.stack([np.cos(angle), np.sin(angle)]) * scale
    table = np.broadcast_to(table[:, None], (2, SUBLANES, ng)).astype(np.float32)
    wyh, wyl = constant_split(np.ascontiguousarray(constant_matrix(ng).T))
    wxh, wxl = constant_split(constant_matrix(nx))
    constants = [upper.astype(BF16), table, wyh, wyl, wxh, wxl]
    vmem = pl.BlockSpec(memory_space=pltpu.VMEM)
    anywhere = pl.BlockSpec(memory_space=pl.ANY)
    dma = pltpu.SemaphoreType.DMA
    result = pl.pallas_call(
        lambda *refs: fused_body(n_dev, *refs),
        in_specs=[anywhere, anywhere] + [vmem] * 8,
        out_specs=vmem,
        out_shape=jax.ShapeDtypeStruct((nr, 2 * nl, per), F32),
        scratch_shapes=[
            pltpu.VMEM((two, nl, zs, ng, nx), F32),
            pltpu.VMEM((two, nr, zs, ng, nx), F32),
            pltpu.VMEM((2, zs, 2 * nl * pitch, nx), F32),
            pltpu.VMEM((nr, 2, chips, n_dev // 2, 2 * nl, LANES), F32),
            pltpu.VMEM((nr, chips, n_dev // 2, 2 * nl, LANES), F32),
            pltpu.VMEM((nr, chips - 1, n_dev // 2, 2 * nl, LANES), F32),
            pltpu.VMEM((nr, 2, n_dev // 2, 2 * nl, LANES), F32),
            pltpu.VMEM((chips, n_dev, LANES), jnp.int32),
            pltpu.VMEM((chips, n_dev, LANES), jnp.int32),
            pltpu.VMEM((chips, n_dev, zs, LANES), F32),
            pltpu.VMEM((chips, n_dev, zs, LANES), F32),
            pltpu.VMEM((n_dev, 2, per // LANES, LANES), jnp.int32),
            dma((2,)),
            dma((own * spans,)),
            dma((own * spans,)),
            dma((nr,)),
            dma((nr,)),
            dma((nr, chips - 1)),
            dma((nr, chips - 1)),
            dma((nr,)),
            dma((nr,)),
        ],
        compiler_params=pltpu.CompilerParams(
            collective_id=0, has_side_effects=True, vmem_limit_bytes=60 * 1024 * 1024
        ),
    )(
        left_bands, right_bands, sphere_index.reshape(-1, LANES), position,
        *[jnp.asarray(c) for c in constants],
    )
    return result.transpose(1, 0, 2).reshape(2, nl, nr, per)


def local(left_bands, right_bands, sphere_index, right_order):
    n_dev = lax.axis_size("grid")
    if fused_fits(left_bands, right_bands, sphere_index, n_dev):
        return fused(left_bands, right_bands, sphere_index, right_order)
    me = lax.axis_index("grid")
    nl, zs, ng, nx = left_bands.shape[1:]
    own_right = right_bands.shape[1]
    rows = ng // n_dev
    other = swapped(right_bands, "band")
    chosen, slot = plan(sphere_index, ng, nx, n_dev)
    filled = chosen >= 0
    col = jnp.where(filled, chosen % (rows * nx), -1)
    kz = chosen // (rows * nx)
    plane = me * zs + jnp.arange(zs, dtype=jnp.int32)
    angle = (plane[None, :, None] * kz[:, None, :] % ng).astype(F32) * (2.0 * math.pi / ng)
    scale = 1.0 / (ng * ng * nx) ** 0.5
    cos_z, sin_z = jnp.cos(angle) * scale, jnp.sin(angle) * scale
    wx, wy = complex_matrix(nx), complex_matrix(ng)

    early = 2 if n_dev == 1 << (n_dev.bit_length() - 1) and n_dev >= 4 else 0

    def partial(right, beside):
        nr = right.shape[1]
        l0, l1 = left_bands[0][:, None], left_bands[1][:, None]
        r0, r1 = right[0][None], right[1][None]
        pair = jnp.stack([l0 * r0 + l1 * r1, l0 * r1 - l1 * r0])
        pair = pair.reshape(2, nl * nr, zs, ng, nx)
        pair = jnp.einsum("cpzyx,cxdk->dpzyk", pair, wx, precision=HIGH)
        if beside is not None and early:
            beside, pair = lax.optimization_barrier((halved(beside, me, n_dev, 0), pair))
        pair = jnp.einsum("cpzyk,cydq->dpzqk", pair, wy, precision=HIGH)
        if beside is not None and early:
            beside, pair = lax.optimization_barrier((halved(beside, me, n_dev, 1), pair))
        return select_sum(pair, col, cos_z, sin_z), beside

    first, _ = partial(right_bands, None)
    first, other = lax.optimization_barrier((first, other))
    second, first = partial(other, first)
    halves = []
    for part, done in ((first, early), (second, 0)):
        got = summed_over_grid(part, me, n_dev, done)
        got = got.transpose(1, 0, 2).reshape(2, nl, own_right, -1)
        halves.append(got)
    result = jnp.concatenate(halves, axis=2)
    own_slot = lax.dynamic_index_in_dim(slot, me, 0, keepdims=False)
    place = jnp.arange(result.shape[3], dtype=jnp.int32)
    pick = (place[:, None] == own_slot[None, :]).astype(F32)
    result = jnp.einsum("dnmt,ti->dnmi", result, pick, precision=HIGHEST)
    position = (right_order - lax.axis_index("band") * own_right) % right_order.shape[0]
    return jnp.take(result, position, axis=2)


def solution(mesh):
    placed = (P(None, "band", "grid", None, None), P(None, "band", "grid", None, None), P(), P())
    return jax.shard_map(
        local, mesh=mesh, in_specs=placed, out_specs=P(None, "band", None, "grid"), check_vma=False
    )
```

```python
import math

import jax
import jax.numpy as jnp
import numpy as np
from jax import lax
from jax.experimental import pallas as pl
from jax.experimental.pallas import tpu as pltpu
from jax.sharding import PartitionSpec as P

HIGH = lax.Precision.HIGH
HIGHEST = lax.Precision.HIGHEST
F32 = jnp.float32
BF16 = jnp.bfloat16


def swapped(block, axis):
    count = lax.axis_size(axis)
    return lax.ppermute(block, axis, [(k, k ^ 1) for k in range(count)])


def dft_tables(length):
    counter = jnp.arange(length, dtype=jnp.int32)
    angles = (counter[:, None] * counter[None, :] % length).astype(F32) * (2.0 * math.pi / length)
    return (jnp.cos(angles), jnp.sin(angles))


def complex_matrix(length):
    cosine, sine = dft_tables(length)
    return jnp.concatenate(
        [jnp.concatenate([cosine, -sine], 1), jnp.concatenate([sine, cosine], 1)], 0
    ).reshape(2, length, 2, length)


def split(value):
    high = lax.reduce_precision(value, 8, 7)
    return high.astype(BF16), (value - high).astype(BF16)


def plan(sphere_index, grid, nx, n_dev):
    rows = grid // n_dev
    per = sphere_index.shape[0] // n_dev
    slots = max(1, per // n_dev)
    wave_z = sphere_index // (grid * nx)
    wave_y = sphere_index // nx % grid
    wave_x = sphere_index % nx
    source = (wave_y // rows).reshape(n_dev, per)
    onehot = (source[:, :, None] == jnp.arange(n_dev, dtype=jnp.int32)).astype(BF16)
    before = jnp.tril(jnp.ones((per, per), BF16), -1)
    counts = jnp.einsum("ij,bjs->bis", before, onehot, preferred_element_type=F32)
    rank = jnp.sum(counts * onehot, axis=2).astype(jnp.int32)
    slot = source * slots + rank
    column = (wave_y % rows) * nx + wave_x
    packed = (wave_z * (rows * nx) + column).reshape(n_dev, per)
    target = jnp.arange(n_dev * slots, dtype=jnp.int32)
    chosen = jnp.sum(
        jnp.where(slot[:, :, None] == target[None, None, :], packed[:, :, None] + 1, 0), axis=1
    ) - 1
    bits = n_dev.bit_length() - 1
    if n_dev == 1 << bits:
        chosen = chosen.reshape((2,) * bits + (n_dev * slots,))
        chosen = chosen.transpose(tuple(range(bits))[::-1] + (bits,))
    chosen = chosen.reshape(n_dev, n_dev, slots).transpose(1, 0, 2).reshape(n_dev, n_dev * slots)
    return chosen, slot


def select_body(field_ref, col_ref, cos_ref, sin_ref, out_ref, parts_ref):
    count, rows, nx = field_ref.shape
    planes = cos_ref.shape[1]
    points = col_ref.shape[2]
    flat = field_ref.reshape(count * rows, nx)
    for row in range(rows):
        value = flat[pl.ds(row, count, stride=rows), :]
        high = value.astype(BF16)
        low = (value - high.astype(F32)).astype(BF16)
        parts_ref[0:count, row * nx : (row + 1) * nx] = high
        parts_ref[count : 2 * count, row * nx : (row + 1) * nx] = low
    tile = min(points, 256)

    def step(index, carry):
        span = pl.ds(pl.multiple_of(index * tile, tile), tile)
        col = col_ref[0, :, span]
        place = lax.broadcasted_iota(jnp.int32, (rows * nx, tile), 0)
        hot = jnp.where(place == col, 1.0, 0.0).astype(BF16)
        both = jnp.dot(parts_ref[...], hot, preferred_element_type=F32)
        got = (both[:count] + both[count:]).reshape(2, count // (2 * planes), planes, tile)
        cosine, sine = cos_ref[0, :, span][None], sin_ref[0, :, span][None]
        real = jnp.sum(got[0] * cosine + got[1] * sine, axis=1)
        imag = jnp.sum(got[1] * cosine - got[0] * sine, axis=1)
        out_ref[0, :, span] = jnp.concatenate([real, imag], axis=0)
        return carry

    lax.fori_loop(0, points // tile, step, 0)


def select_sum(field, col, cos_z, sin_z):
    two, pairs, planes, ng, nx = field.shape
    groups, points = col.shape
    rows = ng // groups
    if rows % 8 == 0 and planes % 8 == 0 and nx % 128 == 0 and points % 256 == 0:
        count = two * pairs * planes
        flops = 4 * count * rows * nx * points * groups
        return pl.pallas_call(
            select_body,
            grid=(groups,),
            in_specs=[
                pl.BlockSpec((count, rows, nx), lambda g: (0, g, 0)),
                pl.BlockSpec((1, 1, points), lambda g: (g, 0, 0)),
                pl.BlockSpec((1, planes, points), lambda g: (g, 0, 0)),
                pl.BlockSpec((1, planes, points), lambda g: (g, 0, 0)),
            ],
            out_specs=pl.BlockSpec((1, 2 * pairs, points), lambda g: (g, 0, 0)),
            out_shape=jax.ShapeDtypeStruct((groups, 2 * pairs, points), F32),
            scratch_shapes=[pltpu.VMEM((2 * count, rows * nx), BF16)],
            cost_estimate=pl.CostEstimate(
                flops=flops, bytes_accessed=4 * count * ng * nx, transcendentals=0
            ),
        )(field.reshape(count, ng, nx), col[:, None, :], cos_z, sin_z)
    high, low = split(field.reshape(2, pairs, planes, groups, rows * nx))
    place = jnp.arange(rows * nx, dtype=jnp.int32)[None, :, None]
    hot = (place == col[:, None, :]).astype(BF16)
    form = "dpzsc,scq->sdpzq"
    got = jnp.einsum(form, high, hot, preferred_element_type=F32) + jnp.einsum(
        form, low, hot, preferred_element_type=F32
    )
    c, s = cos_z[:, None], sin_z[:, None]
    real = jnp.sum(got[:, 0] * c + got[:, 1] * s, axis=2)
    imag = jnp.sum(got[:, 1] * c - got[:, 0] * s, axis=2)
    return jnp.concatenate([real, imag], axis=1)


def halved(part, me, n_dev, bit):
    half = part.shape[2] // 2
    lower, upper = part[:, :, :half], part[:, :, half:]
    mine = me // (1 << bit) % 2 == 1
    route = [(k, k ^ (1 << bit)) for k in range(n_dev)]
    arrived = lax.ppermute(jnp.where(mine, lower, upper), "grid", route)
    return jnp.where(mine, upper, lower) + arrived


def summed_over_grid(part, me, n_dev, done):
    bits = n_dev.bit_length() - 1
    if n_dev == 1 << bits:
        for bit in range(done, bits):
            part = halved(part, me, n_dev, bit)
        return part
    groups, values, points = part.shape
    part = part.reshape(groups, values, n_dev, points // n_dev).transpose(2, 0, 1, 3)
    return lax.psum_scatter(part, "grid", scatter_dimension=0, tiled=False)


LANES = 128
SUBLANES = 8
MESH = pl.DeviceIdType.MESH


def constant_matrix(length):
    counter = np.arange(length)
    angles = (counter[:, None] * counter[None, :] % length) * (2.0 * math.pi / length)
    cosine, sine = np.cos(angles), np.sin(angles)
    return np.concatenate(
        [np.concatenate([cosine, -sine], 1), np.concatenate([sine, cosine], 1)], 0
    ).astype(np.float32)


def constant_split(value):
    high = value.astype(BF16)
    return high, (value - high.astype(np.float32)).astype(BF16)


def dot(a, b):
    return jnp.dot(a, b, preferred_element_type=F32)


def parts(value):
    high = value.astype(BF16)
    return high, (value - high.astype(F32)).astype(BF16)


def lane_gather(value, index):
    return jnp.take_along_axis(value, index, axis=1, mode="promise_in_bounds")


def fused_body(
    n_dev,
    left_hbm, right_hbm, order_ref, *refs,
):
    small_hbm, out_ref, small, refs = refs[:7], refs[7], refs[8:15], refs[15:]
    index_ref, upper_ref, table_ref, wyh, wyl, wxh, wxl = small
    (
    left, right, field, acc, came, came2, final, plan_kx, plan_ky, cos_z, sin_z, own_slot,
    picked, sem_in, sem_xs, sem_xr, sem_1s, sem_1r, sem_2s, sem_2r, sem_3s, sem_3r,
    ) = refs
    nl, planes, ng, nx = left.shape[1:]
    own = right_hbm.shape[1]
    nr = right.shape[1]
    rows = ng // n_dev
    chips = n_dev // 2
    pitch = field.shape[2] // (2 * nl)
    slots = LANES // 2
    blocks = index_ref.shape[0] // n_dev
    me = lax.axis_index("grid")
    band = lax.axis_index("band")
    core, chip = lax.rem(me, 2), me // 2
    partner = me + 1 - 2 * core

    def at(grid):
        return {"grid": grid, "band": band}

    barrier = pltpu.get_barrier_semaphore()
    pl.semaphore_signal(
        barrier, inc=1, device_id={"grid": me, "band": 1 - band}, device_id_type=MESH
    )
    pl.semaphore_signal(barrier, inc=1, device_id=at(partner), device_id_type=MESH)
    for o in range(1, chips):
        other = lax.rem(chip + o, chips) * 2 + core
        pl.semaphore_signal(barrier, inc=1, device_id=at(other), device_id_type=MESH)
    load_right = pltpu.make_async_copy(right_hbm, right.at[:, 0:own], sem_in.at[0])
    load_left = pltpu.make_async_copy(left_hbm, left, sem_in.at[1])
    loads = [
        pltpu.make_async_copy(src, dst, sem_in.at[2 + k])
        for k, (src, dst) in enumerate(zip(small_hbm, small))
    ]
    for load in loads[:1] + [load_right, load_left] + loads[1:]:
        load.start()
    pl.semaphore_wait(barrier, chips + 1)

    def remote(src, dst, send, recv, where):
        return pltpu.make_async_remote_copy(
            src_ref=src, dst_ref=dst, send_sem=send, recv_sem=recv,
            device_id=where, device_id_type=MESH,
        )

    def swap(m, z):
        part = pl.ds(z, 1)
        k = m * planes + z
        return remote(
            right_hbm.at[:, m, part], right.at[:, own + m, part],
            sem_xs.at[k], sem_xr.at[k], {"grid": me, "band": 1 - band},
        )

    for m in range(own):
        for z in range(planes):
            swap(m, z).start()

    bit_x, bit_y = nx.bit_length() - 1, ng.bit_length() - 1
    bit_r = rows.bit_length() - 1
    iota_s = lax.broadcasted_iota(jnp.int32, (n_dev, LANES), 0)
    iota_r = lax.broadcasted_iota(jnp.int32, (slots, LANES), 0)
    iota_p = lax.broadcasted_iota(jnp.int32, (planes, LANES), 0)

    def plan_block(t):
        value = index_ref[pl.ds(pl.multiple_of(t * blocks, blocks), blocks), :]
        source = (value >> (bit_x + bit_r)) & (n_dev - 1)
        ky = (value >> bit_x) & (rows - 1)
        kx = value & (nx - 1)
        kz = value >> (bit_x + bit_y)
        masks = [
            jnp.broadcast_to(source[c : c + 1], (n_dev, LANES)) == iota_s for c in range(blocks)
        ]
        hot = jnp.concatenate([jnp.where(k, 1.0, 0.0) for k in masks], 0).astype(BF16)
        prefix = dot(hot, upper_ref[...])
        carry = jnp.zeros((n_dev, LANES), F32)
        left_side, right_side, ranks = [], [], []
        for c in range(blocks):
            mine = prefix[c * n_dev : (c + 1) * n_dev]
            count = mine[:, :LANES] + carry
            carry = carry + mine[:, LANES:]
            rank = jnp.sum(jnp.where(masks[c], count, 0.0), axis=0, keepdims=True)
            rank = rank.astype(jnp.int32)
            ranks.append(rank)
            wide = [
                jnp.where(
                    masks[c],
                    jnp.broadcast_to(v[c : c + 1].astype(F32), (n_dev, LANES)), 0.0
                )
                for v in (kz, ky, kx)
            ]
            left_side.append(jnp.concatenate(wide, 0))
            right_side.append(
                jnp.where(jnp.broadcast_to(rank, (slots, LANES)) == iota_r, 1.0, 0.0)
            )
        own_slot[t, 0] = source
        own_slot[t, 1] = jnp.concatenate(ranks, 0)
        a = jnp.concatenate(left_side, 1).astype(BF16)
        b = jnp.concatenate(right_side, 1).astype(BF16)
        return lax.dot_general(a, b, (((1,), (1,)), ((), ())), preferred_element_type=F32)

    def plan_chip(ch, carry):
        both = jnp.concatenate([plan_block(2 * ch), plan_block(2 * ch + 1)], 1)
        both = both.astype(jnp.int32)
        kz = both[0:n_dev]
        plan_ky[ch] = both[n_dev : 2 * n_dev]
        plan_kx[ch] = both[2 * n_dev : 3 * n_dev]
        for g in range(n_dev):
            turn = jnp.broadcast_to(kz[g : g + 1], (planes, LANES)) * (me * planes + iota_p)
            turn = turn & (ng - 1)
            cos_z[ch, g] = lane_gather(table_ref[0], turn)
            sin_z[ch, g] = lane_gather(table_ref[1], turn)
        return carry

    def transform(m, z, q, buf):
        r0, r1 = right[0, m, z], right[1, m, z]
        real, imag = [], []
        for e in range(2):
            l0, l1 = left[0, 2 * q + e, z], left[1, 2 * q + e, z]
            real.append(l0 * r0 + l1 * r1)
            imag.append(l0 * r1 - l1 * r0)
        pair = jnp.concatenate([jnp.concatenate(real, 1), jnp.concatenate(imag, 1)], 0)
        high, low = parts(pair)
        y = dot(wyh[...], high) + dot(wyl[...], high) + dot(wyh[...], low)
        lines = jnp.concatenate(
            [
                jnp.concatenate([y[:ng, e * nx : (e + 1) * nx], y[ng:, e * nx : (e + 1) * nx]], 1)
                for e in range(2)
            ],
            0,
        )
        high, low = parts(lines)
        x = dot(high, wxh[...]) + dot(low, wxh[...]) + dot(high, wxl[...])
        for d in range(2):
            for e in range(2):
                start = pl.multiple_of((d * nl + 2 * q + e) * pitch, SUBLANES)
                field[buf, z, pl.ds(start, ng), :] = x[
                    e * ng : (e + 1) * ng, d * nx : (d + 1) * nx
                ]

    sign = jnp.where(lax.broadcasted_iota(jnp.int32, (2 * nl, LANES), 0) < nl, 1.0, -1.0)

    def choose(items, bits):
        for bit in bits:
            items = [jnp.where(bit, items[2 * k + 1], items[2 * k]) for k in range(len(items) // 2)]
        return items[0]

    def bits_of(value, count, shape):
        value = jnp.broadcast_to(value, shape)
        return [((value >> i) & 1) == 1 for i in range(count)]

    def gather_group(m, g, buf, zs, add):
        half, inner = g // (n_dev // 2), lax.rem(g, n_dev // 2)
        shape = (2 * nl, LANES)
        for ch in range(chips):
            index = jnp.broadcast_to(plan_kx[ch, pl.ds(g, 1), :], shape)
            bits = bits_of(plan_ky[ch, pl.ds(g, 1), :], bit_r, shape)
            even = odd = None
            for z in zs:
                got = choose(
                    [
                        lane_gather(
                            field[buf, z, pl.ds(g * rows + k, 2 * nl, stride=pitch), :], index
                        )
                        for k in range(rows)
                    ],
                    bits,
                )
                c = jnp.broadcast_to(cos_z[ch, g, pl.ds(z, 1), :], shape)
                s = jnp.broadcast_to(sin_z[ch, g, pl.ds(z, 1), :], shape)
                even = got * c if even is None else even + got * c
                odd = got * s if odd is None else odd + got * s
            total = even + sign * pltpu.roll(odd, nl, 0)
            if add:
                total = total + acc[m, half, ch, inner]
            acc[m, half, ch, inner] = total

    wide = 2 * LANES
    place = lax.broadcasted_iota(jnp.int32, (nx, wide), 0)

    def matrix_group(m, g, buf, zs):
        half, inner = g // (n_dev // 2), lax.rem(g, n_dev // 2)
        size = 2 * nl
        lines = jnp.concatenate(
            [
                jnp.concatenate(
                    [field[buf, z, pl.ds(g * rows + k, size, stride=pitch), :] for z in zs], 0
                )
                for k in range(rows)
            ],
            1,
        )
        lines = jnp.concatenate(parts(lines), 0)
        count = size * len(zs)
        for pair in range(chips // 2):
            kx = jnp.concatenate([plan_kx[2 * pair + e, pl.ds(g, 1), :] for e in range(2)], 1)
            ky = jnp.concatenate([plan_ky[2 * pair + e, pl.ds(g, 1), :] for e in range(2)], 1)
            hot = jnp.concatenate(
                [
                    jnp.where(
                        place == jnp.broadcast_to(jnp.where(ky == k, kx, -1), (nx, wide)), 1.0, 0.0
                    ).astype(BF16)
                    for k in range(rows)
                ],
                0,
            )
            found = dot(lines, hot)
            found = found[:count] + found[count:]
            for e in range(2):
                ch = 2 * pair + e
                even = odd = None
                for k, z in enumerate(zs):
                    got = found[k * size : (k + 1) * size, e * LANES : (e + 1) * LANES]
                    c = jnp.broadcast_to(cos_z[ch, g, pl.ds(z, 1), :], got.shape)
                    s = jnp.broadcast_to(sin_z[ch, g, pl.ds(z, 1), :], got.shape)
                    even = got * c if even is None else even + got * c
                    odd = got * s if odd is None else odd + got * s
                acc[m, half, ch, inner] = even + sign * pltpu.roll(odd, nl, 0)

    def send1(m):
        return remote(
            acc.at[m, 1 - core], came.at[m], sem_1s.at[m], sem_1r.at[m], at(partner)
        )

    def send2(m, o):
        other = lax.rem(chip + o, chips)
        return remote(
            acc.at[m, core, other], came2.at[m, o - 1],
            sem_2s.at[m, o - 1], sem_2r.at[m, o - 1], at(other * 2 + core),
        )

    def send3(m):
        return remote(
            final.at[m, core], final.at[m, core], sem_3s.at[m], sem_3r.at[m], at(partner)
        )

    def stage2(m):
        send1(m).wait_recv()

        def add(ch, carry):
            acc[m, core, ch] = acc[m, core, ch] + came[m, ch]
            return carry

        lax.fori_loop(0, chips, add, 0)
        for o in range(1, chips):
            send2(m, o).start()

    def stage3(m):
        for o in range(1, chips):
            send2(m, o).wait_recv()
        total = acc[m, core, chip]
        for o in range(1, chips):
            total = total + came2[m, o - 1]
        final[m, core] = total
        send3(m).start()

    for load in loads + [load_right, load_left]:
        load.wait()
    half = nl // 2
    middle = n_dev // 2

    def start(ch, carry):
        plan_chip(ch, carry)
        for q in range(half):
            transform(0, ch, q, 0)
        return carry

    lax.fori_loop(0, planes, start, 0)
    every = range(planes)

    def four(m, k, buf):
        for e in range(3):
            gather_group(m, 4 * k + e, buf, every, False)
        matrix_group(m, 4 * k + 3, buf, every)

    def first(k, carry):
        four(0, k, 0)
        for e in range(2):
            for q in range(half):
                transform(1, 2 * k + e, q, 1)
        return carry

    lax.fori_loop(0, n_dev // 4, first, 0)
    send1(0).start()

    def second(k, carry):
        for e in range(2):
            swap(0, 2 * k + e).wait_recv()
        four(1, k, 1)
        for e in range(2):
            for q in range(half):
                transform(2, 2 * k + e, q, 0)
        return carry

    lax.fori_loop(0, n_dev // 4, second, 0)
    send1(1).start()
    stage2(0)

    def third(z, carry):
        swap(1, z).wait_recv()
        four(2, z, 0)
        for q in range(half):
            transform(3, z, q, 1)
        return carry

    lax.fori_loop(0, 4, third, 0)
    send1(2).start()
    stage2(1)
    stage3(0)

    def fourth(z, carry):
        swap(1, 4 + z).wait_recv()

        def run(q, carry):
            for e in range(4):
                gather_group(3, 8 * z + 4 * q + e, 1, range(4), False)
            transform(3, 4 + z, q, 1)
            return carry

        return lax.fori_loop(0, half, run, carry)

    lax.fori_loop(0, 2, fourth, 0)
    stage2(2)
    stage3(1)
    swap(1, 6).wait_recv()

    def fifth(q, carry):
        for e in range(middle):
            gather_group(3, middle * q + e, 1, (4, 5), True)
        transform(3, 6, q, 1)
        return carry

    lax.fori_loop(0, half, fifth, 0)
    stage3(2)
    swap(1, 7).wait_recv()

    def sixth(q, carry):
        for e in range(middle):
            gather_group(3, middle * q + e, 1, (6,), True)
        transform(3, 7, q, 1)
        return carry

    lax.fori_loop(0, half, sixth, 0)
    for e in range(middle):
        gather_group(3, middle * (1 - core) + e, 1, (7,), True)
    send1(3).start()
    for e in range(middle):
        gather_group(3, middle * core + e, 1, (7,), True)
    stage2(3)

    def pick(m):
        source, rank = own_slot[me, 0], own_slot[me, 1]
        shape = (2 * nl, LANES)
        for c in range(blocks):
            index = jnp.broadcast_to(rank[c : c + 1] + core * slots, shape)
            bits = bits_of(source[c : c + 1], n_dev.bit_length() - 1, shape)
            picked[m, c] = choose(
                [lane_gather(final[m, g // middle, g % middle], index) for g in range(n_dev)],
                bits,
            )

    for m in range(nr - 1):
        send3(m).wait_recv()
        pick(m)
    stage3(3)
    send3(3).wait_recv()
    pick(3)
    for j in range(nr):
        order = lax.rem(order_ref[j] + nr - band * own, nr)
        for c in range(blocks):
            value = picked[0, c]
            for m in range(1, nr):
                value = jnp.where(order == m, picked[m, c], value)
            out_ref[j, :, c * LANES : (c + 1) * LANES] = value

    for m in range(own):
        for z in range(planes):
            swap(m, z).wait_send()
    for m in range(nr):
        send1(m).wait_send()
        for o in range(1, chips):
            send2(m, o).wait_send()
        send3(m).wait_send()


def fused_fits(left_bands, right_bands, sphere_index, n_dev):
    two, nl, zs, ng, nx = left_bands.shape
    per = sphere_index.shape[0] // n_dev
    return (
        ng == nx == LANES
        and zs * n_dev == ng
        and zs == SUBLANES
        and 2 * nl == SUBLANES
        and right_bands.shape[1] == 2
        and lax.axis_size("band") == 2
        and per == SUBLANES * LANES
        and 2 * (per // n_dev) == LANES
        and n_dev == 2 * SUBLANES
    )


def fused(left_bands, right_bands, sphere_index, right_order):
    n_dev = lax.axis_size("grid")
    two, nl, zs, ng, nx = left_bands.shape
    own = right_bands.shape[1]
    nr = right_order.shape[0]
    chips = n_dev // 2
    per = sphere_index.shape[0] // n_dev
    pitch = ng + SUBLANES
    scale = 1.0 / (ng * ng * nx) ** 0.5
    upper = np.concatenate([np.triu(np.ones((LANES, LANES)), 1), np.ones((LANES, LANES))], 1)
    angle = np.arange(ng) * (2.0 * math.pi / ng)
    table = np.stack([np.cos(angle), np.sin(angle)]) * scale
    table = np.broadcast_to(table[:, None], (2, SUBLANES, ng)).astype(np.float32)
    wyh, wyl = constant_split(np.ascontiguousarray(constant_matrix(ng).T))
    wxh, wxl = constant_split(constant_matrix(nx))
    constants = [jnp.asarray(c) for c in (upper.astype(BF16), table, wyh, wyl, wxh, wxl)]
    small = [sphere_index.reshape(-1, LANES)] + constants
    vmem = pl.BlockSpec(memory_space=pltpu.VMEM)
    anywhere = pl.BlockSpec(memory_space=pl.ANY)
    dma = pltpu.SemaphoreType.DMA
    result = pl.pallas_call(
        lambda *refs: fused_body(n_dev, *refs),
        in_specs=[anywhere, anywhere, pl.BlockSpec(memory_space=pltpu.SMEM)] + [anywhere] * 7,
        out_specs=vmem,
        out_shape=jax.ShapeDtypeStruct((nr, 2 * nl, per), F32),
        scratch_shapes=[pltpu.VMEM(c.shape, c.dtype) for c in small] + [
            pltpu.VMEM((two, nl, zs, ng, nx), F32),
            pltpu.VMEM((two, nr, zs, ng, nx), F32),
            pltpu.VMEM((2, zs, 2 * nl * pitch, nx), F32),
            pltpu.VMEM((nr, 2, chips, n_dev // 2, 2 * nl, LANES), F32),
            pltpu.VMEM((nr, chips, n_dev // 2, 2 * nl, LANES), F32),
            pltpu.VMEM((nr, chips - 1, n_dev // 2, 2 * nl, LANES), F32),
            pltpu.VMEM((nr, 2, n_dev // 2, 2 * nl, LANES), F32),
            pltpu.VMEM((chips, n_dev, LANES), jnp.int32),
            pltpu.VMEM((chips, n_dev, LANES), jnp.int32),
            pltpu.VMEM((chips, n_dev, zs, LANES), F32),
            pltpu.VMEM((chips, n_dev, zs, LANES), F32),
            pltpu.VMEM((n_dev, 2, per // LANES, LANES), jnp.int32),
            pltpu.VMEM((nr, per // LANES, 2 * nl, LANES), F32),
            dma((9,)),
            dma((own * zs,)),
            dma((own * zs,)),
            dma((nr,)),
            dma((nr,)),
            dma((nr, chips - 1)),
            dma((nr, chips - 1)),
            dma((nr,)),
            dma((nr,)),
        ],
        compiler_params=pltpu.CompilerParams(
            collective_id=0, has_side_effects=True, vmem_limit_bytes=60 * 1024 * 1024
        ),
    )(
        left_bands, right_bands, right_order, *small,
    )
    return result.transpose(1, 0, 2).reshape(2, nl, nr, per)


def local(left_bands, right_bands, sphere_index, right_order):
    n_dev = lax.axis_size("grid")
    if fused_fits(left_bands, right_bands, sphere_index, n_dev):
        return fused(left_bands, right_bands, sphere_index, right_order)
    me = lax.axis_index("grid")
    nl, zs, ng, nx = left_bands.shape[1:]
    own_right = right_bands.shape[1]
    rows = ng // n_dev
    other = swapped(right_bands, "band")
    chosen, slot = plan(sphere_index, ng, nx, n_dev)
    filled = chosen >= 0
    col = jnp.where(filled, chosen % (rows * nx), -1)
    kz = chosen // (rows * nx)
    plane = me * zs + jnp.arange(zs, dtype=jnp.int32)
    angle = (plane[None, :, None] * kz[:, None, :] % ng).astype(F32) * (2.0 * math.pi / ng)
    scale = 1.0 / (ng * ng * nx) ** 0.5
    cos_z, sin_z = jnp.cos(angle) * scale, jnp.sin(angle) * scale
    wx, wy = complex_matrix(nx), complex_matrix(ng)

    early = 2 if n_dev == 1 << (n_dev.bit_length() - 1) and n_dev >= 4 else 0

    def partial(right, beside):
        nr = right.shape[1]
        l0, l1 = left_bands[0][:, None], left_bands[1][:, None]
        r0, r1 = right[0][None], right[1][None]
        pair = jnp.stack([l0 * r0 + l1 * r1, l0 * r1 - l1 * r0])
        pair = pair.reshape(2, nl * nr, zs, ng, nx)
        pair = jnp.einsum("cpzyx,cxdk->dpzyk", pair, wx, precision=HIGH)
        if beside is not None and early:
            beside, pair = lax.optimization_barrier((halved(beside, me, n_dev, 0), pair))
        pair = jnp.einsum("cpzyk,cydq->dpzqk", pair, wy, precision=HIGH)
        if beside is not None and early:
            beside, pair = lax.optimization_barrier((halved(beside, me, n_dev, 1), pair))
        return select_sum(pair, col, cos_z, sin_z), beside

    first, _ = partial(right_bands, None)
    first, other = lax.optimization_barrier((first, other))
    second, first = partial(other, first)
    halves = []
    for part, done in ((first, early), (second, 0)):
        got = summed_over_grid(part, me, n_dev, done)
        got = got.transpose(1, 0, 2).reshape(2, nl, own_right, -1)
        halves.append(got)
    result = jnp.concatenate(halves, axis=2)
    own_slot = lax.dynamic_index_in_dim(slot, me, 0, keepdims=False)
    place = jnp.arange(result.shape[3], dtype=jnp.int32)
    pick = (place[:, None] == own_slot[None, :]).astype(F32)
    result = jnp.einsum("dnmt,ti->dnmi", result, pick, precision=HIGHEST)
    position = (right_order - lax.axis_index("band") * own_right) % right_order.shape[0]
    return jnp.take(result, position, axis=2)


def solution(mesh):
    placed = (P(None, "band", "grid", None, None), P(None, "band", "grid", None, None), P(), P())
    return jax.shard_map(
        local, mesh=mesh, in_specs=placed, out_specs=P(None, "band", None, "grid"), check_vma=False
    )
```
